256 devices in a mesh: ha: 8 (over z_hi, core), wa: 8 (over z_lo, y), ba: 4 (over x).
Axes of the slice: x: 4, y: 4, z: 8 (z_hi: 4, z_lo: 2; z = z_hi * 2 + z_lo), core: 2. Of those that a mesh axis runs over, the one named last changes fastest.
Arguments:
- tokens: bfloat16 [32, 64, 64, 512], P('ba', 'ha', 'wa'), parts along dimension 0, may hold values from -6 to 6
- norm_gain: float32 [3, 512], replicated, may hold values from 0.1 to 1.9
- w_gatevals: bfloat16 [3, 512, 2048], replicated, may hold values from -0.25 to 0.25
- w_coupling: bfloat16 [3, 512, 128], replicated, may hold values from -0.25 to 0.25
- w_steps: bfloat16 [3, 512, 16], replicated, may hold values from -0.25 to 0.25
- conv_values: float32 [3, 4, 1024], replicated, may hold values from -3 to 3
- conv_coupling: float32 [3, 4, 128], replicated, may hold values from -3 to 3
- step_bias: float32 [3, 16], replicated, may hold values from -4 to 0
- rate_log: float32 [3, 16], replicated, may hold values from -1.5 to 1.5
- skip_gain: float32 [3, 16], replicated, may hold values from 0.5 to 2
- out_gain: float32 [3, 1024], replicated, may hold values from 0.1 to 1.9
- w_output: bfloat16 [3, 1024, 512], replicated, may hold values from -0.1875 to 0.1875
Outputs:
- result: bfloat16 [32, 64, 64, 512], P('ba', 'ha', 'wa'), parts along dimension 0
The draws below stay inside these ranges and needn't reach their ends.
There are 4 independent parts, one for each index of `ba`. The reference program is written for one: setup_inputs(seed, part) draws one part's arguments, and reference() takes and returns one part's arrays. A program takes and returns all parts, laid end to end along the dimension named above; an argument that names none is the same for every part. Nothing has to cross between parts.
All inputs are finite; a program needn't handle non-finite values.
Results may differ from the reference program's by a relative error of at most 0.025.
Values may be sent and summed in bfloat16 or wider, within the bound.
No kernel may reach another device: no remote copies, remote signals or barrier semaphores. Data moves between devices by JAX's collectives and lax.ppermute only.
A program may use at most 128 MiB of HBM per device.

```python
import math
import jax
import jax.numpy as jnp
from jax import lax

D = 512
INNER = 1024
STATE = 64
CONV = 4
LAYERS = 3
FRAMES = 8
HEADS = 16
HEIGHT = 64
WIDTH = 64


def shard_levels(stream_key, dims, shards, smallest, largest):
    def one(dim, shards_of):
        draws = jax.random.uniform(jax.random.fold_in(jax.random.fold_in(stream_key, 6), dim), (shards_of,), jnp.float32, smallest / len(shards), largest / len(shards))
        return jnp.repeat(jnp.exp(draws), dims[dim] // shards_of).reshape((-1,) + (1,) * (len(dims) - dim - 1))

    gain = one(*shards[0])
    for cut in shards[1:]:
        gain = gain * one(*cut)
    return gain


def centred(own_key, extent, scale, limit, shards=(), held_as=jnp.bfloat16):
    factor_of = shard_levels(own_key, extent, shards, -0.22, 0.18) if shards else 1.0
    entries = jax.random.normal(own_key, extent, jnp.float32) * scale * factor_of
    return jnp.minimum(jnp.maximum(entries, -limit), limit).astype(held_as)


def setup_inputs(seed: int = 0, part: int = 0) -> dict:
    keys = jax.random.split(jax.random.key(seed), 13)
    part_keys = jax.random.split(jax.random.fold_in(keys[12], part), 13)
    return {
        "tokens": centred(part_keys[0], (FRAMES, HEIGHT, WIDTH, D), 1.0, 6.0, ((1, 8), (2, 8))),
        "norm_gain": jnp.clip(1.0 + 0.18 * jax.random.normal(keys[1], (LAYERS, D), jnp.float32), 0.1, 1.9),
        "w_gatevals": centred(keys[2], (LAYERS, D, 2 * INNER), D ** -0.5, 0.25),
        "w_coupling": centred(keys[3], (LAYERS, D, 2 * STATE), D ** -0.5, 0.25),
        "w_steps": centred(keys[4], (LAYERS, D, HEADS), D ** -0.5, 0.25),
        "conv_values": centred(keys[5], (LAYERS, CONV, INNER), CONV ** -0.5, 3.0, (), jnp.float32),
        "conv_coupling": centred(keys[6], (LAYERS, CONV, 2 * STATE), CONV ** -0.5, 3.0, (), jnp.float32),
        "step_bias": jnp.clip(jax.random.uniform(keys[7], (LAYERS, HEADS), jnp.float32, -4.0, 0.0), -4.0, 0.0),
        "rate_log": jnp.clip(jax.random.uniform(keys[8], (LAYERS, HEADS), jnp.float32, -1.5, 1.5), -1.5, 1.5),
        "skip_gain": jnp.clip(jax.random.uniform(keys[9], (LAYERS, HEADS), jnp.float32, 0.5, 2.0), 0.5, 2.0),
        "out_gain": jnp.clip(1.0 + 0.18 * jax.random.normal(keys[10], (LAYERS, INNER), jnp.float32), 0.1, 1.9),
        "w_output": centred(keys[11], (LAYERS, INNER, D), INNER ** -0.5, 0.1875),
    }


def causal_conv(values, kernel):
    length = values.shape[1]
    taps = kernel.shape[0]
    padded = jnp.pad(values, ((0, 0), (taps - 1, 0), (0, 0)))
    total = jnp.zeros_like(values)
    for offset in range(taps):
        total = total + padded[:, offset:offset + length, :] * kernel[offset].astype(jnp.float32)
    return total

def mixer(stream, params):
    norm_gain, w_gatevals, w_coupling, w_steps, conv_values, conv_coupling, step_bias, rate_log, skip_gain, out_gain, w_output = params
    count, length, width = stream.shape
    inner = w_gatevals.shape[1] // 2
    states = w_coupling.shape[1] // 2
    heads = w_steps.shape[1]
    headdim = inner // heads
    flat = stream.reshape(count * length, width).astype(jnp.float32)
    normed = (flat * lax.rsqrt(lax.optimization_barrier(jnp.mean(flat * flat, axis=-1, keepdims=True)) + 1e-05) * norm_gain).astype(jnp.bfloat16)
    gatevals = jnp.dot(normed, w_gatevals, preferred_element_type=jnp.float32).astype(jnp.bfloat16)
    coupling = jnp.dot(normed, w_coupling, preferred_element_type=jnp.float32).astype(jnp.bfloat16)
    step_raw = jnp.dot(normed, w_steps, preferred_element_type=jnp.float32)
    gate = gatevals[:, :inner]
    values = gatevals[:, inner:]
    xs = jax.nn.silu(causal_conv(values.astype(jnp.float32).reshape(count, length, inner), conv_values)).astype(jnp.bfloat16)
    maps = jax.nn.silu(causal_conv(coupling.astype(jnp.float32).reshape(count, length, 2 * states), conv_coupling)).astype(jnp.bfloat16)
    input_map = maps[:, :, :states]
    output_map = maps[:, :, states:]
    steps = jax.nn.softplus(step_raw.reshape(count, length, heads) + step_bias)
    cumul = jnp.cumsum(steps * -jnp.exp(rate_log), axis=1).transpose(0, 2, 1)
    steps_heads = steps.transpose(0, 2, 1)
    positions = jnp.arange(length, dtype=jnp.int32)
    lower = positions[:, None] >= positions[None, :]
    spread = cumul[:, :, :, None] - cumul[:, :, None, :]
    decay = jnp.exp(jnp.where(lower[None, None, :, :], spread, -jnp.inf))
    scores = jnp.einsum('ntk,nsk->nts', output_map.astype(jnp.float32), input_map.astype(jnp.float32))
    weights = (scores[:, None, :, :] * decay * steps_heads[:, :, None, :]).astype(jnp.bfloat16)
    heads_in = xs.reshape(count, length, heads, headdim).astype(jnp.float32)
    mixed = jnp.einsum('nhts,nshp->nthp', weights.astype(jnp.float32), heads_in) + skip_gain[:, None] * heads_in
    gated = mixed.reshape(count * length, inner) * jax.nn.silu(gate.astype(jnp.float32))
    normal = (gated * lax.rsqrt(lax.optimization_barrier(jnp.mean(gated * gated, axis=-1, keepdims=True)) + 1e-05) * out_gain).astype(jnp.bfloat16)
    update = jnp.dot(normal, w_output, preferred_element_type=jnp.float32)
    return (flat + update).astype(jnp.bfloat16).reshape(count, length, width)

def sweep(stream, params):
    count, length, width = stream.shape
    block = math.gcd(count, 32)
    grouped = stream.reshape(count // block, block, length, width)
    output = lax.map(lambda piece: mixer(piece, params), grouped)
    return output.reshape(count, length, width)

def reference(tokens, norm_gain, w_gatevals, w_coupling, w_steps, conv_values, conv_coupling, step_bias, rate_log, skip_gain, out_gain, w_output):
    stacked = (norm_gain, w_gatevals, w_coupling, w_steps, conv_values, conv_coupling, step_bias, rate_log, skip_gain, out_gain, w_output)

    def params_of(index):
        return tuple((member[index] for member in stacked))
    frames, rows_all, cols_all, width = tokens.shape
    streams = tokens.transpose(1, 2, 0, 3).reshape(rows_all * cols_all, frames, width)
    current = sweep(streams, params_of(0)).reshape(rows_all, cols_all, frames, width).transpose(2, 0, 1, 3)
    streams = current.transpose(0, 2, 1, 3).reshape(frames * cols_all, rows_all, width)
    current = sweep(streams, params_of(1)).reshape(frames, cols_all, rows_all, width).transpose(0, 2, 1, 3)
    streams = current.reshape(frames * rows_all, cols_all, width)
    current = sweep(streams, params_of(2)).reshape(frames, rows_all, cols_all, width)
    return current
```

```python
import functools

import jax
import jax.numpy as jnp
from jax import lax
from jax.experimental import pallas as pl
from jax.experimental.pallas import tpu as pltpu
from jax.sharding import PartitionSpec as P

LINES = 8
LENGTH = 64
ROWS = LINES * LENGTH
WIDTH = 512
INNER = 1024
HEADS = 16
STATES = 64
STEPS = 4
CHUNK = INNER // STEPS
LANES = 128
LOG2E = 1.4426950408889634
F32 = jnp.float32
BF16 = jnp.bfloat16


def iota(shape, dim):
    return lax.broadcasted_iota(jnp.int32, shape, dim)


def dot(a, b):
    return jnp.dot(a, b, preferred_element_type=F32)


def dot_t(a, b):
    return lax.dot_general(a, b, (((1,), (1,)), ((), ())), preferred_element_type=F32)


def split3(value):
    high = value.astype(BF16)
    rest = value - high.astype(F32)
    middle = rest.astype(BF16)
    low = (rest - middle.astype(F32)).astype(BF16)
    return high, middle, low


def swap_matrix():
    r, c = iota((64, 64), 0), iota((64, 64), 1)
    return ((r // 8 == c % 8) & (r % 8 == c // 8)).astype(BF16)


def half_silu(half):
    return half + half * jnp.tanh(half)


def kernel(
    layer,
    stride,
    x_ref,
    norm_ref,
    wgate_ref,
    wvalue_ref,
    wcoup_ref,
    wsteps_ref,
    taps_ref,
    ctaps_ref,
    bias_ref,
    rate_ref,
    skip_ref,
    ogain_ref,
    wout_hbm,
    out_ref,
    xf,
    normed,
    padded,
    cpadded,
    scores,
    cum,
    rowside,
    skipx,
    gates,
    gated,
    sumsq,
    wout,
    sem,
):
    j = pl.program_id(0)
    pad = 8 if stride == 1 else 24
    span = LENGTH + pad

    row = iota((LENGTH, LANES), 0)
    col = iota((LENGTH, LANES), 1) % LENGTH
    if stride == 1:
        keep = col <= row
    else:
        keep = (col // stride <= row // stride) & (col % stride == row % stride)

    def load_line(s):
        if layer == 0:
            return xf[:, s * 8 : (s + 1) * 8, :].reshape(LENGTH, WIDTH)
        return x_ref[:, s].astype(F32).reshape(LENGTH, WIDTH)

    copy = pltpu.make_async_copy(wout_hbm.at[layer], wout, sem)

    @pl.when(j == 0)
    def _():
        copy.start()
        if layer == 0:
            swap = swap_matrix()
            for f in range(8):
                xf[f] = dot(swap, x_ref[f].astype(F32).reshape(64, WIDTH).astype(BF16))
        gain = norm_ref[layer : layer + 1, :]
        for s in range(LINES):
            x = load_line(s)
            scale = lax.rsqrt(jnp.mean(x * x, axis=-1, keepdims=True) + 1e-05)
            normed[s * LENGTH : (s + 1) * LENGTH, :] = (x * scale * gain).astype(BF16)

        copies = (iota((LANES, HEADS), 0) % HEADS == iota((LANES, HEADS), 1)).astype(BF16)
        wsteps = dot(copies, wsteps_ref[...]).astype(BF16)
        coupling = dot(normed[...], wcoup_ref[...])
        steps_raw = dot_t(normed[...], wsteps)

        padded[...] = jnp.zeros_like(padded)
        cpadded[...] = jnp.zeros_like(cpadded)
        taps = ctaps_ref[...] * 0.5
        for s in range(LINES):
            cpadded[s * span + pad : (s + 1) * span, :] = coupling[s * LENGTH : (s + 1) * LENGTH, :]
        bias = jnp.concatenate([bias_ref[layer : layer + 1, :]] * 8, axis=1)
        rate = jnp.concatenate([-jnp.exp(rate_ref[layer : layer + 1, :]) * LOG2E] * 8, axis=1)
        tri = keep[:, :LENGTH].astype(BF16)
        tri3 = jnp.concatenate([tri] * 3, axis=1)
        lane = iota((LENGTH, LANES), 1)
        for s in range(LINES):
            base = s * span + pad
            half = sum(
                cpadded[base - (3 - k) * stride : base - (3 - k) * stride + LENGTH, :] * taps[k : k + 1, :]
                for k in range(4)
            )
            maps = half_silu(half)
            inputs = maps[:, :STATES].astype(BF16)
            outputs = maps[:, STATES:].astype(BF16)
            scores[s] = dot_t(outputs, jnp.concatenate([inputs, inputs], axis=0))

            raw = steps_raw[s * LENGTH : (s + 1) * LENGTH, :] + bias
            e = jnp.exp(-jnp.abs(raw))
            steps = jnp.maximum(raw, 0.0) + jnp.where(e < 1e-3, e - 0.5 * e * e, jnp.log(1.0 + e))
            total = dot(tri3, jnp.concatenate(split3(steps * rate), axis=0))
            high, middle, low = split3(total)
            cum[s * LENGTH : (s + 1) * LENGTH, :] = jnp.where(
                lane < HEADS, high, jnp.where(lane < 2 * HEADS, middle, low)
            )
            side = total - jnp.log(steps) * LOG2E
            rowside[s] = jnp.transpose(jnp.concatenate([side, side], axis=0))[:HEADS, :]

        spread = (iota((HEADS, INNER), 1) // STATES == iota((HEADS, INNER), 0)).astype(F32)
        skip = jnp.dot(
            jnp.broadcast_to(skip_ref[layer : layer + 1, :], (8, HEADS)),
            spread,
            precision=lax.Precision.HIGHEST,
            preferred_element_type=F32,
        )
        for c in range(STEPS):
            skipx[c] = skip[:, c * CHUNK : (c + 1) * CHUNK]
        sumsq[...] = jnp.zeros_like(sumsq)

    lane3 = iota((LANES, CHUNK), 0)
    expand = (
        (lane3 < 3 * HEADS) & (lane3 % HEADS == 4 * j + iota((LANES, CHUNK), 1) // STATES)
    ).astype(BF16)
    taps = taps_ref[...] * 0.5
    lower = iota((LENGTH, LANES), 1) < STATES
    lower1 = iota((1, LANES), 1) < STATES
    zero = jnp.zeros((LENGTH, LANES), BF16)
    for b in range(2):
        rows = slice(b * 256, (b + 1) * 256)
        value = dot(normed[rows, :], wvalue_ref[...])
        for q in range(4):
            s = b * 4 + q
            for t in range(2):
                padded[t, s * span + pad : (s + 1) * span, :] = value[
                    q * LENGTH : (q + 1) * LENGTH, t * LANES : (t + 1) * LANES
                ]
        gates[rows, :] = half_silu(dot(normed[rows, :], wgate_ref[...]) * 0.5)
        time_side = dot(cum[rows, :], expand)
        for q in range(4):
            s = b * 4 + q
            here = slice(s * LENGTH, (s + 1) * LENGTH)
            base = s * span + pad
            square = sumsq[here, :]
            for t in range(2):
                lanes = slice(t * LANES, (t + 1) * LANES)
                half = sum(
                    padded[t, base - (3 - k) * stride : base - (3 - k) * stride + LENGTH, :] * taps[k : k + 1, lanes]
                    for k in range(4)
                )
                xs = half_silu(half).astype(BF16)
                head = 4 * j + 2 * t
                side = jnp.where(lower1, rowside[s, pl.ds(head, 1), :], rowside[s, pl.ds(head + 1, 1), :])
                power = jnp.where(keep, time_side[q * LENGTH : (q + 1) * LENGTH, lanes] - side, -jnp.inf)
                weights = (scores[s] * jnp.exp2(power)).astype(BF16)
                pair = jnp.concatenate([jnp.where(lower, xs, zero), jnp.where(lower, zero, xs)], axis=0)
                mixed = dot(weights, pair) + skipx[j, 0:1, lanes] * xs.astype(F32)
                mixed = mixed * gates[here, lanes]
                square = square + mixed * mixed
                gated[j, here, lanes] = (mixed * ogain_ref[layer : layer + 1, lanes]).astype(BF16)
            sumsq[here, :] = square

    @pl.when(j == STEPS - 1)
    def _():
        copy.wait()
        for b in range(2):
            rows = slice(b * 256, (b + 1) * 256)
            update = dot(gated[0, rows, :], wout[0:CHUNK, :])
            for c in range(1, STEPS):
                update = update + dot(gated[c, rows, :], wout[c * CHUNK : (c + 1) * CHUNK, :])
            scale = lax.rsqrt(jnp.sum(sumsq[rows, :], axis=-1, keepdims=True) * (1.0 / INNER) + 1e-05)
            update = update * scale
            for q in range(4):
                s = b * 4 + q
                y = load_line(s) + update[q * LENGTH : (q + 1) * LENGTH, :]
                if layer == 0:
                    out_ref[:, s] = y.reshape(8, 8, WIDTH).astype(BF16)
                elif layer == 1:
                    xf[:, s * 8 : (s + 1) * 8, :] = y.reshape(8, 8, WIDTH)
                else:
                    out_ref[s] = y.reshape(8, 8, WIDTH).astype(BF16)
        if layer == 1:
            swap = swap_matrix()
            for i in range(8):
                turned = dot(swap, xf[i].astype(BF16))
                out_ref[:, i] = turned.reshape(8, 8, WIDTH).astype(BF16)


def mixer(x, layer, params):
    stride = 8 if layer == 0 else 1
    pad = 8 if stride == 1 else 24
    span = LENGTH + pad

    def whole(shape):
        return pl.BlockSpec(shape, lambda j: (0,) * len(shape))

    in_specs = [
        whole((8, 8, 8, WIDTH)),
        whole((3, WIDTH)),
        pl.BlockSpec((None, WIDTH, CHUNK), lambda j: (layer, 0, j)),
        pl.BlockSpec((None, WIDTH, CHUNK), lambda j: (layer, 0, STEPS + j)),
        pl.BlockSpec((None, WIDTH, 2 * STATES), lambda j: (layer, 0, 0)),
        pl.BlockSpec((None, HEADS, WIDTH), lambda j: (layer, 0, 0)),
        pl.BlockSpec((None, 4, CHUNK), lambda j: (layer, 0, j)),
        pl.BlockSpec((None, 4, 2 * STATES), lambda j: (layer, 0, 0)),
        whole((3, HEADS)),
        whole((3, HEADS)),
        whole((3, HEADS)),
        pl.BlockSpec((3, CHUNK), lambda j: (0, j)),
        pl.BlockSpec(memory_space=pl.ANY),
    ]
    scratch = [
        pltpu.VMEM((8, 64, WIDTH), F32),
        pltpu.VMEM((ROWS, WIDTH), BF16),
        pltpu.VMEM((2, LINES * span, LANES), F32),
        pltpu.VMEM((LINES * span, LANES), F32),
        pltpu.VMEM((LINES, LENGTH, LANES), F32),
        pltpu.VMEM((ROWS, LANES), BF16),
        pltpu.VMEM((LINES, HEADS, LANES), F32),
        pltpu.VMEM((STEPS, 8, CHUNK), F32),
        pltpu.VMEM((ROWS, CHUNK), F32),
        pltpu.VMEM((STEPS, ROWS, CHUNK), BF16),
        pltpu.VMEM((ROWS, LANES), F32),
        pltpu.VMEM((INNER, WIDTH), BF16),
        pltpu.SemaphoreType.DMA,
    ]
    if layer == 0:
        x, *params = (pltpu.with_memory_space_constraint(p, pltpu.HBM) for p in (x, *params))
    (norm_gain, w_gatevals, w_coupling, w_steps, conv_values, conv_coupling,
     step_bias, rate_log, skip_gain, out_gain, w_output) = params
    return pl.pallas_call(
        functools.partial(kernel, layer, stride),
        grid=(STEPS,),
        in_specs=in_specs,
        out_specs=whole((8, 8, 8, WIDTH)),
        out_shape=jax.ShapeDtypeStruct((8, 8, 8, WIDTH), BF16),
        scratch_shapes=scratch,
        name=f"mixer{layer}",
        compiler_params=pltpu.CompilerParams(dimension_semantics=("arbitrary",), vmem_limit_bytes=24 * 2**20),
        cost_estimate=pl.CostEstimate(flops=2_000_000_000, bytes_accessed=5_000_000, transcendentals=2_000_000),
    )(x, norm_gain, w_gatevals, w_gatevals, w_coupling, w_steps, conv_values, conv_coupling,
      step_bias, rate_log, skip_gain, out_gain, w_output)


def shards(tokens, *params):
    params = params[:3] + (jnp.swapaxes(params[3], 1, 2),) + params[4:]
    current = mixer(tokens, 0, params)
    current = lax.all_to_all(current, "ha", split_axis=0, concat_axis=0, tiled=True)
    current = mixer(current, 1, params)
    current = lax.all_to_all(current, "wa", split_axis=0, concat_axis=0, tiled=True)
    current = mixer(current, 2, params)
    current = current.reshape(64, 8, WIDTH)
    current = lax.all_to_all(current, ("ha", "wa"), split_axis=0, concat_axis=0, tiled=True)
    return current.reshape(8, 8, 8, WIDTH)


def solution(mesh):
    spec = P("ba", "ha", "wa", None)
    return jax.shard_map(shards, mesh=mesh, in_specs=(spec,) + (P(),) * 11, out_specs=spec, check_vma=False)
```

```python
import functools

import jax
import jax.numpy as jnp
from jax import lax
from jax.experimental import pallas as pl
from jax.experimental.pallas import tpu as pltpu
from jax.sharding import PartitionSpec as P

LINES = 8
LENGTH = 64
ROWS = LINES * LENGTH
WIDTH = 512
INNER = 1024
HEADS = 16
STATES = 64
STEPS = 4
CHUNK = INNER // STEPS
LANES = 128
BLOCKS = 1
BLOCK = ROWS // BLOCKS
WHOLE = (True, False, False, False, False, False, True, True, True, True, False)
LOG2E = 1.4426950408889634
F32 = jnp.float32
BF16 = jnp.bfloat16


def iota(shape, dim):
    return lax.broadcasted_iota(jnp.int32, shape, dim)


def dot(a, b):
    return jnp.dot(a, b, preferred_element_type=F32)


def dot_t(a, b):
    return lax.dot_general(a, b, (((1,), (1,)), ((), ())), preferred_element_type=F32)


def split3(value):
    high = value.astype(BF16)
    rest = value - high.astype(F32)
    middle = rest.astype(BF16)
    low = (rest - middle.astype(F32)).astype(BF16)
    return high, middle, low


def swap_matrix():
    r, c = iota((64, 64), 0), iota((64, 64), 1)
    return ((r // 8 == c % 8) & (r % 8 == c // 8)).astype(BF16)


def half_silu(half):
    return half + half * jnp.tanh(half)


def kernel(layer, stride, *refs):
    (x_in, *given) = refs[:12]
    out_ref = refs[12]
    (xf, normed, padded, cpadded, scores, cum, rowside, skipx, gates, gated, sumsq, total_ref) = refs[13:25]
    if layer == 0:
        held, sems = refs[25:37], refs[37]
        sources = [x_in] + [ref if small else ref.at[layer] for ref, small in zip(given, WHOLE)]
        copies = [pltpu.make_async_copy(src, dst, sems.at[n]) for n, (src, dst) in enumerate(zip(sources, held))]
        for n in (0, 1, 3, 4, 6, 7, 8, 9, 5, 10, 2, 11):
            copies[n].start()
        x_ref, *views = held
    else:
        x_ref, views = x_in, [ref if small else ref.at[layer] for ref, small in zip(given, WHOLE)]

    def wait(*which):
        if layer == 0:
            for n in which:
                copies[n].wait()

    norm_ref, w_ref, wcoup_ref, wsteps_ref, taps_ref, ctaps_ref, bias_ref, rate_ref, skip_ref, ogain_ref, wout = views
    pad = 8 if stride == 1 else 24
    span = LENGTH + pad

    row = iota((LENGTH, LANES), 0)
    col = iota((LENGTH, LANES), 1) % LENGTH
    if stride == 1:
        keep = col <= row
    else:
        keep = (col // stride <= row // stride) & (col % stride == row % stride)

    def load_line(s):
        if layer == 0:
            return xf[:, s * 8 : (s + 1) * 8, :].reshape(LENGTH, WIDTH)
        return x_ref[:, s].astype(F32).reshape(LENGTH, WIDTH)

    wait(0, 1)
    if layer == 0:
        swap = swap_matrix()
        for f in range(8):
            xf[f] = dot(swap, x_ref[f].astype(F32).reshape(64, WIDTH).astype(BF16))
    gain = norm_ref[layer : layer + 1, :] * 0.5
    for s in range(LINES):
        x = load_line(s)
        scale = lax.rsqrt(jnp.mean(x * x, axis=-1, keepdims=True) + 1e-05)
        normed[s * LENGTH : (s + 1) * LENGTH, :] = (x * scale * gain).astype(BF16)

    wait(3, 4, 6, 7, 8, 9)
    spread16 = jnp.where(iota((HEADS, LANES), 1) % HEADS == iota((HEADS, LANES), 0), 2.0, 0.0).astype(BF16)
    wsteps = lax.dot_general(
        wsteps_ref[...], spread16, (((0,), (0,)), ((), ())), preferred_element_type=F32
    ).astype(BF16)
    small = dot(normed[...], jnp.concatenate([wcoup_ref[...], wsteps], axis=1))

    for s in range(LINES):
        for t in range(2):
            padded[t, s * span : s * span + pad, :] = jnp.zeros((pad, LANES), F32)
        cpadded[s * span : s * span + pad, :] = jnp.zeros((pad, LANES), F32)
        cpadded[s * span + pad : (s + 1) * span, :] = small[s * LENGTH : (s + 1) * LENGTH, :LANES]
    taps = ctaps_ref[...]
    bias = jnp.concatenate([bias_ref[layer : layer + 1, :]] * 8, axis=1)
    rate = jnp.concatenate([-jnp.exp(rate_ref[layer : layer + 1, :]) * LOG2E] * 8, axis=1)
    tri = keep[:, :LENGTH].astype(BF16)
    tri3 = jnp.concatenate([tri] * 3, axis=1)
    group = iota((LENGTH, LANES), 1) // HEADS
    raw = small[:LENGTH, LANES:]
    for s in range(1, LINES):
        raw = jnp.where(group == s, small[s * LENGTH : (s + 1) * LENGTH, LANES:], raw)
    raw = raw + bias
    e = jnp.exp(-jnp.abs(raw))
    steps = jnp.maximum(raw, 0.0) + jnp.where(e < 1e-3, e - 0.5 * e * e, jnp.log(1.0 + e))
    total = dot(tri3, jnp.concatenate(split3(steps * rate), axis=0))
    high, middle, low = (part.astype(F32) for part in split3(total))
    middle = pltpu.roll(middle, HEADS, 1)
    low = pltpu.roll(low, 2 * HEADS, 1)
    for s in range(LINES):
        parts = jnp.where(
            group == s,
            high,
            jnp.where(group == (s + 1) % 8, middle, jnp.where(group == (s + 2) % 8, low, 0.0)),
        )
        cum[s * LENGTH : (s + 1) * LENGTH, :] = parts.astype(BF16)
    side = total - jnp.log(steps) * LOG2E
    turned = jnp.transpose(jnp.concatenate([side, side], axis=0))
    for s in range(LINES):
        rowside[s] = turned[s * HEADS : (s + 1) * HEADS, :]
    for s in range(LINES):
        base = s * span + pad
        half = sum(
            cpadded[base - (3 - k) * stride : base - (3 - k) * stride + LENGTH, :] * taps[k : k + 1, :]
            for k in range(4)
        )
        maps = half_silu(half)
        inputs = maps[:, :STATES].astype(BF16)
        outputs = maps[:, STATES:].astype(BF16)
        scores[s] = dot_t(outputs, jnp.concatenate([inputs, inputs], axis=0))

    spread = (iota((HEADS, INNER), 1) // STATES == iota((HEADS, INNER), 0)).astype(F32)
    skip = jnp.dot(
        jnp.broadcast_to(skip_ref[layer : layer + 1, :], (8, HEADS)),
        spread,
        precision=lax.Precision.HIGHEST,
        preferred_element_type=F32,
    )
    for c in range(STEPS):
        skipx[c] = skip[:, c * CHUNK : (c + 1) * CHUNK]
    sumsq[...] = jnp.zeros_like(sumsq)
    total_ref[...] = jnp.zeros_like(total_ref)
    gated[1] = jnp.zeros((ROWS, CHUNK), BF16)
    wait(5, 10, 2, 11)

    def project(c, slot, rows):
        first = pl.multiple_of(c * CHUNK, CHUNK)
        return dot(gated[slot, rows, :], wout[pl.ds(first, CHUNK), :])

    def chunk(j, carry):
        start = pl.multiple_of(j * CHUNK, CHUNK)
        lane3 = iota((LANES, CHUNK), 0)
        expand = (lane3 % HEADS == 4 * j + iota((LANES, CHUNK), 1) // STATES).astype(BF16)
        taps = taps_ref[:, pl.ds(start, CHUNK)]
        ogain = ogain_ref[layer : layer + 1, pl.ds(start, CHUNK)]
        wgate = w_ref[:, pl.ds(start, CHUNK)]
        wvalue = w_ref[:, pl.ds(pl.multiple_of(INNER + j * CHUNK, CHUNK), CHUNK)]
        lower = iota((LENGTH, LANES), 1) < STATES
        lower1 = iota((1, LANES), 1) < STATES
        zero = jnp.zeros((LENGTH, LANES), BF16)
        slot = lax.rem(j, 2)
        before = lax.rem(j + 1, 2)
        for b in range(BLOCKS):
            rows = slice(b * BLOCK, (b + 1) * BLOCK)
            value = dot(normed[rows, :], wvalue)
            for q in range(BLOCK // LENGTH):
                s = b * (BLOCK // LENGTH) + q
                for t in range(2):
                    padded[t, s * span + pad : (s + 1) * span, :] = value[
                        q * LENGTH : (q + 1) * LENGTH, t * LANES : (t + 1) * LANES
                    ]
            gates[rows, :] = half_silu(dot(normed[rows, :], wgate))
            time_side = dot(cum[rows, :], expand)
            total_ref[rows, :] += project(jnp.maximum(j - 1, 0), before, rows)
            for q in range(BLOCK // LENGTH):
                s = b * (BLOCK // LENGTH) + q
                here = slice(s * LENGTH, (s + 1) * LENGTH)
                base = s * span + pad
                square = sumsq[here, :]
                for t in range(2):
                    lanes = slice(t * LANES, (t + 1) * LANES)
                    half = sum(
                        padded[t, base - (3 - k) * stride : base - (3 - k) * stride + LENGTH, :] * taps[k : k + 1, lanes]
                        for k in range(4)
                    )
                    silu = half_silu(half)
                    xs = silu.astype(BF16)
                    head = 4 * j + 2 * t
                    side = jnp.where(lower1, rowside[s, pl.ds(head, 1), :], rowside[s, pl.ds(head + 1, 1), :])
                    power = jnp.where(keep, time_side[q * LENGTH : (q + 1) * LENGTH, lanes] - side, -jnp.inf)
                    weights = (scores[s] * jnp.exp2(power)).astype(BF16)
                    pair = jnp.concatenate([jnp.where(lower, xs, zero), jnp.where(lower, zero, xs)], axis=0)
                    mixed = dot(weights, pair) + skipx[j, 0:1, lanes] * silu
                    mixed = mixed * gates[here, lanes]
                    square = square + mixed * mixed
                    gated[slot, here, lanes] = (mixed * ogain[:, lanes]).astype(BF16)
                sumsq[here, :] = square
        return carry

    lax.fori_loop(0, STEPS, chunk, 0)

    for b in range(BLOCKS):
        rows = slice(b * BLOCK, (b + 1) * BLOCK)
        update = total_ref[rows, :] + project(STEPS - 1, (STEPS - 1) % 2, rows)
        scale = lax.rsqrt(jnp.sum(sumsq[rows, :], axis=-1, keepdims=True) * (1.0 / INNER) + 1e-05)
        update = update * scale
        for q in range(BLOCK // LENGTH):
            s = b * (BLOCK // LENGTH) + q
            y = load_line(s) + update[q * LENGTH : (q + 1) * LENGTH, :]
            if layer == 0:
                out_ref[:, s] = y.reshape(8, 8, WIDTH).astype(BF16)
            elif layer == 1:
                xf[:, s * 8 : (s + 1) * 8, :] = y.reshape(8, 8, WIDTH)
            else:
                out_ref[s] = y.reshape(8, 8, WIDTH).astype(BF16)
    if layer == 1:
        swap = swap_matrix()
        for i in range(8):
            turned = dot(swap, xf[i].astype(BF16))
            out_ref[:, i] = turned.reshape(8, 8, WIDTH).astype(BF16)


def mixer(x, layer, params):
    stride = 8 if layer == 0 else 1
    pad = 8 if stride == 1 else 24
    span = LENGTH + pad
    scratch = [
        pltpu.VMEM((8, 64, WIDTH), F32),
        pltpu.VMEM((ROWS, WIDTH), BF16),
        pltpu.VMEM((2, LINES * span, LANES), F32),
        pltpu.VMEM((LINES * span, LANES), F32),
        pltpu.VMEM((LINES, LENGTH, LANES), F32),
        pltpu.VMEM((ROWS, LANES), BF16),
        pltpu.VMEM((LINES, HEADS, LANES), F32),
        pltpu.VMEM((STEPS, 8, CHUNK), F32),
        pltpu.VMEM((ROWS, CHUNK), F32),
        pltpu.VMEM((2, ROWS, CHUNK), BF16),
        pltpu.VMEM((ROWS, LANES), F32),
        pltpu.VMEM((ROWS, WIDTH), F32),
    ]
    space = pltpu.VMEM
    if layer == 0:
        space = pl.ANY
        x, *params = (pltpu.with_memory_space_constraint(p, pltpu.HBM) for p in (x, *params))
        shapes = [p.shape if small else p.shape[1:] for p, small in zip(params, WHOLE)]
        scratch += [pltpu.VMEM(x.shape, BF16)] + [pltpu.VMEM(shape, p.dtype) for shape, p in zip(shapes, params)]
        scratch += [pltpu.SemaphoreType.DMA((12,))]
    return pl.pallas_call(
        functools.partial(kernel, layer, stride),
        in_specs=[pl.BlockSpec(memory_space=space)] * 12,
        out_specs=pl.BlockSpec(memory_space=pltpu.VMEM),
        out_shape=jax.ShapeDtypeStruct((8, 8, 8, WIDTH), BF16),
        scratch_shapes=scratch,
        name=f"mixer{layer}",
        compiler_params=pltpu.CompilerParams(vmem_limit_bytes=24 * 2**20),
        cost_estimate=pl.CostEstimate(flops=2_000_000_000, bytes_accessed=5_000_000, transcendentals=2_000_000),
    )(x, *params)


def shards(tokens, *params):
    params = params[:3] + (jnp.swapaxes(params[3], 1, 2),) + params[4:]
    current = mixer(tokens, 0, params)
    current = lax.all_to_all(current, "ha", split_axis=0, concat_axis=0, tiled=True)
    current = mixer(current, 1, params)
    current = lax.all_to_all(current, "wa", split_axis=0, concat_axis=0, tiled=True)
    current = mixer(current, 2, params)
    current = current.reshape(64, 8, WIDTH)
    current = lax.all_to_all(current, ("ha", "wa"), split_axis=0, concat_axis=0, tiled=True)
    return current.reshape(8, 8, 8, WIDTH)


def solution(mesh):
    spec = P("ba", "ha", "wa", None)
    return jax.shard_map(shards, mesh=mesh, in_specs=(spec,) + (P(),) * 11, out_specs=spec, check_vma=False)
```

```python
import functools

import jax
import jax.numpy as jnp
from jax import lax
from jax.experimental import pallas as pl
from jax.experimental.pallas import tpu as pltpu
from jax.sharding import Mesh
from jax.sharding import PartitionSpec as P

LINES = 8
LENGTH = 64
ROWS = LINES * LENGTH
WIDTH = 512
INNER = 1024
HEADS = 16
STATES = 64
STEPS = 4
CHUNK = INNER // STEPS
LANES = 128
BLOCKS = 1
BLOCK = ROWS // BLOCKS
GIVEN = ((4, 2, 2, 4), (2, 4, 4, 2), (4, 2, 4, 2))
WHOLE = (True, False, False, False, False, False, True, True, True, True, False)
LOG2E = 1.4426950408889634
F32 = jnp.float32
BF16 = jnp.bfloat16


def iota(shape, dim):
    return lax.broadcasted_iota(jnp.int32, shape, dim)


def dot(a, b):
    return jnp.dot(a, b, preferred_element_type=F32)


def dot_t(a, b):
    return lax.dot_general(a, b, (((1,), (1,)), ((), ())), preferred_element_type=F32)


def split3(value):
    high = value.astype(BF16)
    rest = value - high.astype(F32)
    middle = rest.astype(BF16)
    low = (rest - middle.astype(F32)).astype(BF16)
    return high, middle, low


def swap_matrix():
    r, c = iota((64, 64), 0), iota((64, 64), 1)
    return ((r // 8 == c % 8) & (r % 8 == c // 8)).astype(BF16)


def order_matrix():
    r, c = iota((64, 64), 0), iota((64, 64), 1)
    return (c == (r // 4 % 2) * 32 + (r // 8 % 4) * 8 + (r // 32) * 4 + r % 4).astype(BF16)


def half_silu(half):
    return half + half * jnp.tanh(half)


def kernel(layer, stride, *refs):
    (x_in, *given) = refs[:12]
    out_ref = refs[12]
    (xf, normed, padded, cpadded, scores, cum, rowside, skipx, gates, gated, sumsq, total_ref) = refs[13:25]
    if layer == 0:
        held, sems = refs[25:37], refs[37]
        sources = [x_in] + [ref if small else ref.at[layer] for ref, small in zip(given, WHOLE)]
        copies = [pltpu.make_async_copy(src, dst, sems.at[n]) for n, (src, dst) in enumerate(zip(sources, held))]
        for n in (0, 1, 3, 4, 6, 7, 8, 9, 5, 10, 2, 11):
            copies[n].start()
        x_ref, *views = held
    else:
        x_ref, views = x_in, [ref if small else ref.at[layer] for ref, small in zip(given, WHOLE)]

    def wait(*which):
        if layer == 0:
            for n in which:
                copies[n].wait()

    norm_ref, w_ref, wcoup_ref, wsteps_ref, taps_ref, ctaps_ref, bias_ref, rate_ref, skip_ref, ogain_ref, wout = views
    pad = 8 if stride == 1 else 24
    span = LENGTH + pad

    row = iota((LENGTH, LANES), 0)
    col = iota((LENGTH, LANES), 1) % LENGTH
    if stride == 1:
        keep = col <= row
    else:
        keep = (col // stride <= row // stride) & (col % stride == row % stride)

    def load_line(s):
        if layer == 0:
            return xf[:, s * 8 : (s + 1) * 8, :].reshape(LENGTH, WIDTH)
        if layer == 1:
            return x_ref[:, :, s // 4, s % 4].astype(F32).reshape(LENGTH, WIDTH)
        return xf[s]

    for s in range(LINES):
        for t in range(2):
            padded[t, s * span : s * span + pad, :] = jnp.zeros((pad, LANES), F32)
        cpadded[s * span : s * span + pad, :] = jnp.zeros((pad, LANES), F32)
    sumsq[...] = jnp.zeros_like(sumsq)
    total_ref[...] = jnp.zeros_like(total_ref)
    gated[1] = jnp.zeros((ROWS, CHUNK), BF16)

    wait(0, 1)
    if layer == 2:
        order = order_matrix()
        for s in range(LINES):
            line = x_ref[:, :, s // 2, s % 2].astype(F32).reshape(LENGTH, WIDTH)
            xf[s] = dot(order, line.astype(BF16))
    if layer == 0:
        swap = swap_matrix()
        for f in range(8):
            xf[f] = dot(swap, x_ref[f].astype(F32).reshape(64, WIDTH).astype(BF16))
    gain = norm_ref[layer : layer + 1, :] * 0.5
    for s in range(LINES):
        x = load_line(s)
        scale = lax.rsqrt(jnp.mean(x * x, axis=-1, keepdims=True) + 1e-05)
        normed[s * LENGTH : (s + 1) * LENGTH, :] = (x * scale * gain).astype(BF16)

    wait(3, 4, 6, 7, 8, 9)
    spread16 = jnp.where(iota((HEADS, LANES), 1) % HEADS == iota((HEADS, LANES), 0), 2.0, 0.0).astype(BF16)
    wsteps = lax.dot_general(
        wsteps_ref[...], spread16, (((0,), (0,)), ((), ())), preferred_element_type=F32
    ).astype(BF16)
    small = dot(normed[...], jnp.concatenate([wcoup_ref[...], wsteps], axis=1))

    for s in range(LINES):
        cpadded[s * span + pad : (s + 1) * span, :] = small[s * LENGTH : (s + 1) * LENGTH, :LANES]
    taps = ctaps_ref[...]
    bias = jnp.concatenate([bias_ref[layer : layer + 1, :]] * 8, axis=1)
    rate = jnp.concatenate([-jnp.exp(rate_ref[layer : layer + 1, :]) * LOG2E] * 8, axis=1)
    tri = keep[:, :LENGTH].astype(BF16)
    tri3 = jnp.concatenate([tri] * 3, axis=1)
    group = iota((LENGTH, LANES), 1) // HEADS
    raw = small[:LENGTH, LANES:]
    for s in range(1, LINES):
        raw = jnp.where(group == s, small[s * LENGTH : (s + 1) * LENGTH, LANES:], raw)
    raw = raw + bias
    e = jnp.exp(-jnp.abs(raw))
    steps = jnp.maximum(raw, 0.0) + jnp.where(e < 1e-3, e - 0.5 * e * e, jnp.log(1.0 + e))
    total = dot(tri3, jnp.concatenate(split3(steps * rate), axis=0))
    high, middle, low = (part.astype(F32) for part in split3(total))
    middle = pltpu.roll(middle, HEADS, 1)
    low = pltpu.roll(low, 2 * HEADS, 1)
    for s in range(LINES):
        parts = jnp.where(
            group == s,
            high,
            jnp.where(group == (s + 1) % 8, middle, jnp.where(group == (s + 2) % 8, low, 0.0)),
        )
        cum[s * LENGTH : (s + 1) * LENGTH, :] = parts.astype(BF16)
    side = total - jnp.log(steps) * LOG2E
    turned = jnp.transpose(jnp.concatenate([side, side], axis=0))
    for s in range(LINES):
        rowside[s] = turned[s * HEADS : (s + 1) * HEADS, :]
    for s in range(LINES):
        base = s * span + pad
        half = sum(
            cpadded[base - (3 - k) * stride : base - (3 - k) * stride + LENGTH, :] * taps[k : k + 1, :]
            for k in range(4)
        )
        maps = half_silu(half)
        inputs = maps[:, :STATES].astype(BF16)
        outputs = maps[:, STATES:].astype(BF16)
        scores[s] = dot_t(outputs, jnp.concatenate([inputs, inputs], axis=0))

    spread = (iota((HEADS, INNER), 1) // STATES == iota((HEADS, INNER), 0)).astype(F32)
    skip = jnp.dot(
        jnp.broadcast_to(skip_ref[layer : layer + 1, :], (8, HEADS)),
        spread,
        precision=lax.Precision.HIGHEST,
        preferred_element_type=F32,
    )
    for c in range(STEPS):
        skipx[c] = skip[:, c * CHUNK : (c + 1) * CHUNK]
    wait(5, 10, 2, 11)

    def project(c, slot, rows):
        first = pl.multiple_of(c * CHUNK, CHUNK)
        return dot(gated[slot, rows, :], wout[pl.ds(first, CHUNK), :])

    def chunk(j, carry):
        start = pl.multiple_of(j * CHUNK, CHUNK)
        lane3 = iota((LANES, CHUNK), 0)
        expand = (lane3 % HEADS == 4 * j + iota((LANES, CHUNK), 1) // STATES).astype(BF16)
        taps = taps_ref[:, pl.ds(start, CHUNK)]
        ogain = ogain_ref[layer : layer + 1, pl.ds(start, CHUNK)]
        wgate = w_ref[:, pl.ds(start, CHUNK)]
        wvalue = w_ref[:, pl.ds(pl.multiple_of(INNER + j * CHUNK, CHUNK), CHUNK)]
        lower = iota((LENGTH, LANES), 1) < STATES
        lower1 = iota((1, LANES), 1) < STATES
        zero = jnp.zeros((LENGTH, LANES), BF16)
        slot = lax.rem(j, 2)
        before = lax.rem(j + 1, 2)
        for b in range(BLOCKS):
            rows = slice(b * BLOCK, (b + 1) * BLOCK)
            value = dot(normed[rows, :], wvalue)
            for q in range(BLOCK // LENGTH):
                s = b * (BLOCK // LENGTH) + q
                for t in range(2):
                    padded[t, s * span + pad : (s + 1) * span, :] = value[
                        q * LENGTH : (q + 1) * LENGTH, t * LANES : (t + 1) * LANES
                    ]
            gates[rows, :] = half_silu(dot(normed[rows, :], wgate))
            time_side = dot(cum[rows, :], expand)
            total_ref[rows, :] += project(jnp.maximum(j - 1, 0), before, rows)
            for q in range(BLOCK // LENGTH):
                s = b * (BLOCK // LENGTH) + q
                here = slice(s * LENGTH, (s + 1) * LENGTH)
                base = s * span + pad
                square = sumsq[here, :]
                for t in range(2):
                    lanes = slice(t * LANES, (t + 1) * LANES)
                    half = sum(
                        padded[t, base - (3 - k) * stride : base - (3 - k) * stride + LENGTH, :] * taps[k : k + 1, lanes]
                        for k in range(4)
                    )
                    silu = half_silu(half)
                    xs = silu.astype(BF16)
                    head = 4 * j + 2 * t
                    side = jnp.where(lower1, rowside[s, pl.ds(head, 1), :], rowside[s, pl.ds(head + 1, 1), :])
                    power = jnp.where(keep, time_side[q * LENGTH : (q + 1) * LENGTH, lanes] - side, -jnp.inf)
                    weights = (scores[s] * jnp.exp2(power)).astype(BF16)
                    pair = jnp.concatenate([jnp.where(lower, xs, zero), jnp.where(lower, zero, xs)], axis=0)
                    mixed = dot(weights, pair) + skipx[j, 0:1, lanes] * silu
                    mixed = mixed * gates[here, lanes]
                    square = square + mixed * mixed
                    gated[slot, here, lanes] = (mixed * ogain[:, lanes]).astype(BF16)
                sumsq[here, :] = square
        return carry

    lax.fori_loop(0, STEPS, chunk, 0)

    for b in range(BLOCKS):
        rows = slice(b * BLOCK, (b + 1) * BLOCK)
        update = total_ref[rows, :] + project(STEPS - 1, (STEPS - 1) % 2, rows)
        scale = lax.rsqrt(jnp.sum(sumsq[rows, :], axis=-1, keepdims=True) * (1.0 / INNER) + 1e-05)
        update = update * scale
        for q in range(BLOCK // LENGTH):
            s = b * (BLOCK // LENGTH) + q
            y = load_line(s) + update[q * LENGTH : (q + 1) * LENGTH, :]
            if layer == 0:
                out_ref[:, s // 4, :, s % 4] = y.reshape(4, 2, 8, WIDTH).astype(BF16)
            elif layer == 1:
                xf[:, s * 8 : (s + 1) * 8, :] = y.reshape(8, 8, WIDTH)
            else:
                out_ref[s // 2, :, :, s % 2] = y.reshape(2, 4, 8, WIDTH).astype(BF16)
    if layer == 1:
        swap = swap_matrix()
        for i in range(8):
            turned = dot(swap, xf[i].astype(BF16))
            out_ref[i % 2, :, i // 2] = turned.reshape(4, 2, 8, WIDTH).astype(BF16)


def mixer(x, layer, params):
    stride = 8 if layer == 0 else 1
    pad = 8 if stride == 1 else 24
    span = LENGTH + pad
    scratch = [
        pltpu.VMEM((8, 64, WIDTH), F32),
        pltpu.VMEM((ROWS, WIDTH), BF16),
        pltpu.VMEM((2, LINES * span, LANES), F32),
        pltpu.VMEM((LINES * span, LANES), F32),
        pltpu.VMEM((LINES, LENGTH, LANES), F32),
        pltpu.VMEM((ROWS, LANES), BF16),
        pltpu.VMEM((LINES, HEADS, LANES), F32),
        pltpu.VMEM((STEPS, 8, CHUNK), F32),
        pltpu.VMEM((ROWS, CHUNK), F32),
        pltpu.VMEM((2, ROWS, CHUNK), BF16),
        pltpu.VMEM((ROWS, LANES), F32),
        pltpu.VMEM((ROWS, WIDTH), F32),
    ]
    space = pltpu.VMEM
    if layer == 0:
        space = pl.ANY
        x, *params = (pltpu.with_memory_space_constraint(p, pltpu.HBM) for p in (x, *params))
        shapes = [p.shape if small else p.shape[1:] for p, small in zip(params, WHOLE)]
        scratch += [pltpu.VMEM(x.shape, BF16)] + [pltpu.VMEM(shape, p.dtype) for shape, p in zip(shapes, params)]
        scratch += [pltpu.SemaphoreType.DMA((12,))]
    return pl.pallas_call(
        functools.partial(kernel, layer, stride),
        in_specs=[pl.BlockSpec(memory_space=space)] * 12,
        out_specs=pl.BlockSpec(memory_space=pltpu.VMEM),
        out_shape=jax.ShapeDtypeStruct(GIVEN[layer] + (8, WIDTH), BF16),
        scratch_shapes=scratch,
        name=f"mixer{layer}",
        compiler_params=pltpu.CompilerParams(vmem_limit_bytes=24 * 2**20),
        cost_estimate=pl.CostEstimate(flops=2_000_000_000, bytes_accessed=5_000_000, transcendentals=2_000_000),
    )(x, *params)


def shards(tokens, *params):
    params = params[:3] + (jnp.swapaxes(params[3], 1, 2),) + params[4:]
    current = tokens
    for layer, axes in enumerate((("zh", "core", "zl"), ("core", "y"), ("zh", "zl", "y"))):
        current = mixer(current, layer, params)
        shape = current.shape
        current = current.reshape(lax.axis_size(axes), -1, WIDTH)
        current = lax.all_to_all(current, axes, split_axis=0, concat_axis=0, tiled=True).reshape(shape)
    return current.reshape(8, 8, 8, WIDTH)


def solution(mesh):
    mesh = Mesh(mesh.devices.reshape(4, 2, 2, 4, 4), ("zh", "core", "zl", "y", "x"))
    spec = P("x", ("zh", "core"), ("zl", "y"), None)
    return jax.shard_map(shards, mesh=mesh, in_specs=(spec,) + (P(),) * 11, out_specs=spec, check_vma=False)
```

```python
import functools

import jax
import jax.numpy as jnp
from jax import lax
from jax.experimental import pallas as pl
from jax.experimental.pallas import tpu as pltpu
from jax.sharding import Mesh
from jax.sharding import PartitionSpec as P

LINES = 8
LENGTH = 64
ROWS = LINES * LENGTH
WIDTH = 512
INNER = 1024
HEADS = 16
STATES = 64
STEPS = 4
CHUNK = INNER // STEPS
LANES = 128
BLOCKS = 1
BLOCK = ROWS // BLOCKS
GIVEN = ((4, 2, 2, 4), (2, 4, 4, 2), (4, 2, 4, 2))
WHOLE = (True, False, False, False, False, False, True, True, True, True, False)
LOG2E = 1.4426950408889634
F32 = jnp.float32
BF16 = jnp.bfloat16


def iota(shape, dim):
    return lax.broadcasted_iota(jnp.int32, shape, dim)


def dot(a, b):
    return jnp.dot(a, b, preferred_element_type=F32)


def dot_t(a, b):
    return lax.dot_general(a, b, (((1,), (1,)), ((), ())), preferred_element_type=F32)


def split3(value):
    high = value.astype(BF16)
    rest = value - high.astype(F32)
    middle = rest.astype(BF16)
    low = (rest - middle.astype(F32)).astype(BF16)
    return high, middle, low


def swap_matrix():
    r, c = iota((64, 64), 0), iota((64, 64), 1)
    return ((r // 8 == c % 8) & (r % 8 == c // 8)).astype(BF16)


def order_matrix():
    r, c = iota((64, 64), 0), iota((64, 64), 1)
    return (c == (r // 4 % 2) * 32 + (r // 8 % 4) * 8 + (r // 32) * 4 + r % 4).astype(BF16)


def half_silu(half):
    return half + half * jnp.tanh(half)


def kernel(layer, stride, *refs):
    (x_in, *given) = refs[:12]
    out_ref = refs[12]
    (xf, normed, padded, cpadded, scores, cum, rowside, skipx, gates, gated, sumsq, total_ref) = refs[13:25]
    if layer == 0:
        held, sems = refs[25:37], refs[37]
        sources = [x_in] + [ref if small else ref.at[layer] for ref, small in zip(given, WHOLE)]
        copies = [pltpu.make_async_copy(src, dst, sems.at[n]) for n, (src, dst) in enumerate(zip(sources, held))]
        for n in (0, 1, 3, 4, 6, 7, 8, 9, 5, 10, 2, 11):
            copies[n].start()
        x_ref, *views = held
    else:
        x_ref, views = x_in, [ref if small else ref.at[layer] for ref, small in zip(given, WHOLE)]

    def wait(*which):
        if layer == 0:
            for n in which:
                copies[n].wait()

    norm_ref, w_ref, wcoup_ref, wsteps_ref, taps_ref, ctaps_ref, bias_ref, rate_ref, skip_ref, ogain_ref, wout = views
    pad = 8 if stride == 1 else 24
    span = LENGTH + pad

    row = iota((LENGTH, LANES), 0)
    col = iota((LENGTH, LANES), 1) % LENGTH
    if stride == 1:
        keep = col <= row
    else:
        keep = (col // stride <= row // stride) & (col % stride == row % stride)

    def load_line(s):
        if layer == 0:
            return xf[:, s * 8 : (s + 1) * 8, :].reshape(LENGTH, WIDTH)
        if layer == 1:
            return x_ref[:, :, s // 4, s % 4].astype(F32).reshape(LENGTH, WIDTH)
        return xf[s]

    for s in range(LINES):
        for t in range(2):
            for slot in range(2):
                padded[slot, t, s * span : s * span + pad, :] = jnp.zeros((pad, LANES), F32)
        cpadded[s * span : s * span + pad, :] = jnp.zeros((pad, LANES), F32)
    sumsq[...] = jnp.zeros_like(sumsq)
    total_ref[...] = jnp.zeros_like(total_ref)
    gated[1] = jnp.zeros((ROWS, CHUNK), BF16)

    wait(0, 1)
    if layer == 2:
        order = order_matrix()
        for s in range(LINES):
            line = x_ref[:, :, s // 2, s % 2].astype(F32).reshape(LENGTH, WIDTH)
            xf[s] = dot(order, line.astype(BF16))
    if layer == 0:
        swap = swap_matrix()
        for f in range(8):
            xf[f] = dot(swap, x_ref[f].astype(F32).reshape(64, WIDTH).astype(BF16))
    gain = norm_ref[layer : layer + 1, :] * 0.5
    for s in range(LINES):
        x = load_line(s)
        scale = lax.rsqrt(jnp.mean(x * x, axis=-1, keepdims=True) + 1e-05)
        normed[s * LENGTH : (s + 1) * LENGTH, :] = (x * scale * gain).astype(BF16)

    wait(3, 4, 6, 7, 8, 9)
    spread16 = jnp.where(iota((HEADS, LANES), 1) % HEADS == iota((HEADS, LANES), 0), 2.0, 0.0).astype(BF16)
    wsteps = lax.dot_general(
        wsteps_ref[...], spread16, (((0,), (0,)), ((), ())), preferred_element_type=F32
    ).astype(BF16)
    small = dot(normed[...], jnp.concatenate([wcoup_ref[...], wsteps], axis=1))

    def produce(c, slot):
        wgate = w_ref[:, pl.ds(c * CHUNK, CHUNK)]
        wvalue = w_ref[:, pl.ds(INNER + c * CHUNK, CHUNK)]
        value = dot(normed[...], wvalue)
        for s in range(LINES):
            for t in range(2):
                padded[slot, t, s * span + pad : (s + 1) * span, :] = value[
                    s * LENGTH : (s + 1) * LENGTH, t * LANES : (t + 1) * LANES
                ]
        gates[slot] = half_silu(dot(normed[...], wgate))

    wait(5, 10, 2, 11)
    produce(0, 0)
    for s in range(LINES):
        cpadded[s * span + pad : (s + 1) * span, :] = small[s * LENGTH : (s + 1) * LENGTH, :LANES]
    taps = ctaps_ref[...]
    bias = jnp.concatenate([bias_ref[layer : layer + 1, :]] * 8, axis=1)
    rate = jnp.concatenate([-jnp.exp(rate_ref[layer : layer + 1, :]) * LOG2E] * 8, axis=1)
    tri = keep[:, :LENGTH].astype(BF16)
    tri3 = jnp.concatenate([tri] * 3, axis=1)
    group = iota((LENGTH, LANES), 1) // HEADS
    raw = small[:LENGTH, LANES:]
    for s in range(1, LINES):
        raw = jnp.where(group == s, small[s * LENGTH : (s + 1) * LENGTH, LANES:], raw)
    raw = raw + bias
    e = jnp.exp(-jnp.abs(raw))
    steps = jnp.maximum(raw, 0.0) + jnp.where(e < 1e-3, e - 0.5 * e * e, jnp.log(1.0 + e))
    total = dot(tri3, jnp.concatenate(split3(steps * rate), axis=0))
    high, middle, low = (part.astype(F32) for part in split3(total))
    middle = pltpu.roll(middle, HEADS, 1)
    low = pltpu.roll(low, 2 * HEADS, 1)
    for s in range(LINES):
        parts = jnp.where(
            group == s,
            high,
            jnp.where(group == (s + 1) % 8, middle, jnp.where(group == (s + 2) % 8, low, 0.0)),
        )
        cum[s * LENGTH : (s + 1) * LENGTH, :] = parts.astype(BF16)
    side = total - jnp.log(steps) * LOG2E
    turned = jnp.transpose(jnp.concatenate([side, side], axis=0))
    for s in range(LINES):
        rowside[s] = turned[s * HEADS : (s + 1) * HEADS, :]
    for s in range(LINES):
        base = s * span + pad
        half = sum(
            cpadded[base - (3 - k) * stride : base - (3 - k) * stride + LENGTH, :] * taps[k : k + 1, :]
            for k in range(4)
        )
        maps = half_silu(half)
        inputs = maps[:, :STATES].astype(BF16)
        outputs = maps[:, STATES:].astype(BF16)
        scores[s] = dot_t(outputs, jnp.concatenate([inputs, inputs], axis=0))

    spread = (iota((HEADS, INNER), 1) // STATES == iota((HEADS, INNER), 0)).astype(F32)
    skip = jnp.dot(
        jnp.broadcast_to(skip_ref[layer : layer + 1, :], (8, HEADS)),
        spread,
        precision=lax.Precision.HIGHEST,
        preferred_element_type=F32,
    )
    for c in range(STEPS):
        skipx[c] = skip[:, c * CHUNK : (c + 1) * CHUNK]
    def project(c, slot, rows):
        first = c * CHUNK
        return dot(gated[slot, rows, :], wout[pl.ds(first, CHUNK), :])

    def chunk(j, slot):
        start = j * CHUNK
        lane3 = iota((LANES, CHUNK), 0)
        expand = (lane3 % HEADS == 4 * j + iota((LANES, CHUNK), 1) // STATES).astype(BF16)
        taps = taps_ref[:, pl.ds(start, CHUNK)]
        ogain = ogain_ref[layer : layer + 1, pl.ds(start, CHUNK)]
        lower = iota((LENGTH, LANES), 1) < STATES
        lower1 = iota((1, LANES), 1) < STATES
        zero = jnp.zeros((LENGTH, LANES), BF16)
        before = 1 - slot
        if j + 1 < STEPS:
            produce(j + 1, before)
        for b in range(BLOCKS):
            rows = slice(b * BLOCK, (b + 1) * BLOCK)
            time_side = dot(cum[rows, :], expand)
            if j > 0:
                total_ref[rows, :] += project(j - 1, before, rows)
            for q in range(BLOCK // LENGTH):
                s = b * (BLOCK // LENGTH) + q
                here = slice(s * LENGTH, (s + 1) * LENGTH)
                base = s * span + pad
                square = sumsq[here, :]
                for t in range(2):
                    lanes = slice(t * LANES, (t + 1) * LANES)
                    half = sum(
                        padded[slot, t, base - (3 - k) * stride : base - (3 - k) * stride + LENGTH, :] * taps[k : k + 1, lanes]
                        for k in range(4)
                    )
                    silu = half_silu(half)
                    xs = silu.astype(BF16)
                    head = 4 * j + 2 * t
                    side = jnp.where(lower1, rowside[s, pl.ds(head, 1), :], rowside[s, pl.ds(head + 1, 1), :])
                    power = jnp.where(keep, time_side[q * LENGTH : (q + 1) * LENGTH, lanes] - side, -jnp.inf)
                    weights = (scores[s] * jnp.exp2(power)).astype(BF16)
                    pair = jnp.concatenate([jnp.where(lower, xs, zero), jnp.where(lower, zero, xs)], axis=0)
                    mixed = dot(weights, pair) + skipx[j, 0:1, lanes] * silu
                    mixed = mixed * gates[slot, here, lanes]
                    square = square + mixed * mixed
                    gated[slot, here, lanes] = (mixed * ogain[:, lanes]).astype(BF16)
                sumsq[here, :] = square

    for j in range(STEPS):
        chunk(j, j % 2)

    for b in range(BLOCKS):
        rows = slice(b * BLOCK, (b + 1) * BLOCK)
        update = total_ref[rows, :] + project(STEPS - 1, (STEPS - 1) % 2, rows)
        scale = lax.rsqrt(jnp.sum(sumsq[rows, :], axis=-1, keepdims=True) * (1.0 / INNER) + 1e-05)
        update = update * scale
        for q in range(BLOCK // LENGTH):
            s = b * (BLOCK // LENGTH) + q
            y = load_line(s) + update[q * LENGTH : (q + 1) * LENGTH, :]
            if layer == 0:
                out_ref[:, s // 4, :, s % 4] = y.reshape(4, 2, 8, WIDTH).astype(BF16)
            elif layer == 1:
                xf[:, s * 8 : (s + 1) * 8, :] = y.reshape(8, 8, WIDTH)
            else:
                out_ref[s // 2, :, :, s % 2] = y.reshape(2, 4, 8, WIDTH).astype(BF16)
    if layer == 1:
        swap = swap_matrix()
        for i in range(8):
            turned = dot(swap, xf[i].astype(BF16))
            out_ref[i % 2, :, i // 2] = turned.reshape(4, 2, 8, WIDTH).astype(BF16)


def mixer(x, layer, params):
    stride = 8 if layer == 0 else 1
    pad = 8 if stride == 1 else 24
    span = LENGTH + pad
    scratch = [
        pltpu.VMEM((8, 64, WIDTH), F32),
        pltpu.VMEM((ROWS, WIDTH), BF16),
        pltpu.VMEM((2, 2, LINES * span, LANES), F32),
        pltpu.VMEM((LINES * span, LANES), F32),
        pltpu.VMEM((LINES, LENGTH, LANES), F32),
        pltpu.VMEM((ROWS, LANES), BF16),
        pltpu.VMEM((LINES, HEADS, LANES), F32),
        pltpu.VMEM((STEPS, 8, CHUNK), F32),
        pltpu.VMEM((2, ROWS, CHUNK), F32),
        pltpu.VMEM((2, ROWS, CHUNK), BF16),
        pltpu.VMEM((ROWS, LANES), F32),
        pltpu.VMEM((ROWS, WIDTH), F32),
    ]
    space = pltpu.VMEM
    if layer == 0:
        space = pl.ANY
        x, *params = (pltpu.with_memory_space_constraint(p, pltpu.HBM) for p in (x, *params))
        shapes = [p.shape if small else p.shape[1:] for p, small in zip(params, WHOLE)]
        scratch += [pltpu.VMEM(x.shape, BF16)] + [pltpu.VMEM(shape, p.dtype) for shape, p in zip(shapes, params)]
        scratch += [pltpu.SemaphoreType.DMA((12,))]
    return pl.pallas_call(
        functools.partial(kernel, layer, stride),
        in_specs=[pl.BlockSpec(memory_space=space)] * 12,
        out_specs=pl.BlockSpec(memory_space=pltpu.VMEM),
        out_shape=jax.ShapeDtypeStruct(GIVEN[layer] + (8, WIDTH), BF16),
        scratch_shapes=scratch,
        name=f"mixer{layer}",
        compiler_params=pltpu.CompilerParams(vmem_limit_bytes=24 * 2**20),
        cost_estimate=pl.CostEstimate(flops=2_000_000_000, bytes_accessed=5_000_000, transcendentals=2_000_000),
    )(x, *params)


def shards(tokens, *params):
    params = params[:3] + (jnp.swapaxes(params[3], 1, 2),) + params[4:]
    current = tokens
    for layer, axes in enumerate((("zh", "core", "zl"), ("core", "y"), ("zh", "zl", "y"))):
        current = mixer(current, layer, params)
        shape = current.shape
        current = current.reshape(lax.axis_size(axes), -1, WIDTH)
        current = lax.all_to_all(current, axes, split_axis=0, concat_axis=0, tiled=True).reshape(shape)
    return current.reshape(8, 8, 8, WIDTH)


def solution(mesh):
    mesh = Mesh(mesh.devices.reshape(4, 2, 2, 4, 4), ("zh", "core", "zl", "y", "x"))
    spec = P("x", ("zh", "core"), ("zl", "y"), None)
    return jax.shard_map(shards, mesh=mesh, in_specs=(spec,) + (P(),) * 11, out_specs=spec, check_vma=False)
```
